32 devices in a mesh: ctx: 8 (over z, x), tp: 4 (over y, core).
Axes of the slice: x: 2, y: 2, z: 4, core: 2. Of those that a mesh axis runs over, the one named last changes fastest.
Arguments:
- hidden_in: bfloat16 [4096, 5376], P(('ctx', 'tp')), may hold values from -6 to 6
- stretch_start: int32 [1], replicated, may hold values from 1 to 1024
- pre_gain: float32 [5376], replicated, may hold values from 0.1 to 1.9
- q_weight: bfloat16 [5376, 4096], P('ctx', 'tp'), may hold values from -1 to 1
- k_weight: bfloat16 [5376, 2048], P('ctx', 'tp'), may hold values from -1 to 1
- v_weight: bfloat16 [5376, 2048], P('ctx', 'tp'), may hold values from -0.078125 to 0.078125
- o_weight: bfloat16 [4096, 5376], P('tp', 'ctx'), may hold values from -0.09375 to 0.09375
- q_gain: float32 [128], replicated, may hold values from 0.5 to 5
- k_gain: float32 [128], replicated, may hold values from 0.5 to 5
- prior_keys: bfloat16 [1024, 2048], P(None, 'tp'), may hold values from -6 to 6
- prior_values: bfloat16 [1024, 2048], P(None, 'tp'), may hold values from -6 to 6
- post_gain: float32 [5376], replicated, may hold values from 0.1 to 1.9
Outputs:
- result: bfloat16 [4096, 5376], P(('ctx', 'tp'))
The draws below stay inside these ranges and needn't reach their ends.
All inputs are finite; a program needn't handle non-finite values.
Results may differ from the reference program's by a relative error of at most 0.013.
Values may be sent and summed in bfloat16 or wider, within the bound.
No kernel may reach another device: no remote copies, remote signals or barrier semaphores. Data moves between devices by JAX's collectives and lax.ppermute only.
A program may use at most 128 MiB of HBM per device.

```python
import jax
import jax.numpy as jnp
from jax import lax

D = 5376
HEADS = 32
KVH = 16
HD = 128
WINDOW = 1024
TOK_DEV = 512
TOKENS = 4096


def query_base(key):
    normal_q = jax.random.normal(jax.random.fold_in(key, 11), (D, HEADS * HD), jnp.float32)
    return jnp.clip(normal_q, -6.0, 6.0) / jnp.sqrt(jnp.float32(D))


def draw_q_weight(key, part):
    return query_base(key).astype(jnp.bfloat16)


def draw_k_weight(key, part):
    normal_k = jax.random.normal(jax.random.fold_in(key, 12), (D, KVH * HD), jnp.float32)
    own_part = jnp.clip(normal_k, -6.0, 6.0) / jnp.sqrt(jnp.float32(D))
    return own_part.astype(jnp.bfloat16)


def gain_draw(key, salt):
    unit = jax.random.uniform(jax.random.fold_in(key, salt), (HD,), jnp.float32)
    return jnp.exp(jnp.log(0.6) + unit * (jnp.log(1.6) - jnp.log(0.6)))


def draw_q_gain(key, part):
    return gain_draw(key, 21)


def draw_k_gain(key, part):
    return gain_draw(key, 22)


def shard_levels(key, shape, shards, low, high):
    factor_of, own = 1.0, jax.random.fold_in(key, 6)
    for dim, parts in shards:
        draws = jnp.exp(jax.random.uniform(jax.random.fold_in(own, dim), (parts,), jnp.float32, low / len(shards), high / len(shards)))
        factor_of = factor_of * jnp.repeat(draws, shape[dim] // parts).reshape([-1 if axis == dim else 1 for axis in range(len(shape))])
    return factor_of


def centred(key, dims, scale, most, shards=(), held_as=jnp.bfloat16):
    array = jax.random.normal(key, dims, jnp.float32) * scale
    if len(shards) > 0:
        array = shard_levels(key, dims, shards, -0.22, 0.18) * array
    return jnp.clip(array, min=-most, max=most).astype(held_as)


def setup_inputs(seed: int = 0) -> dict:
    seeds = jax.random.split(jax.random.key(seed), 13)
    return {
        "hidden_in": centred(seeds[0], (TOKENS, D), 1.0, 6.0, ((0, 32),)),
        "stretch_start": jax.random.randint(seeds[1], (1,), 1, WINDOW + 1).astype(jnp.int32),
        "pre_gain": jnp.clip(1.0 + 0.18 * jax.random.normal(seeds[2], (D,), jnp.float32), 0.1, 1.9),
        "q_weight": draw_q_weight(jax.random.fold_in(seeds[12], 71), 0),
        "k_weight": draw_k_weight(jax.random.fold_in(seeds[12], 71), 0),
        "v_weight": centred(seeds[5], (D, KVH * HD), D ** -0.5, 0.078125, ((0, 8), (1, 4))),
        "o_weight": centred(seeds[6], (HEADS * HD, D), (HEADS * HD) ** -0.5, 0.09375, ((0, 4), (1, 8))),
        "q_gain": draw_q_gain(jax.random.fold_in(seeds[12], 71), 0),
        "k_gain": draw_k_gain(jax.random.fold_in(seeds[12], 71), 0),
        "prior_keys": centred(seeds[9], (WINDOW, KVH * HD), 1.0, 6.0, ((1, 4),)),
        "prior_values": centred(seeds[10], (WINDOW, KVH * HD), 1.0, 6.0, ((1, 4),)),
        "post_gain": jnp.clip(1.0 + 0.18 * jax.random.normal(seeds[11], (D,), jnp.float32), 0.1, 1.9),
    }


EPSILON = 1e-06
QUERY_FACTOR = 168.0 ** (-0.5)

def rms_scale(inputs, scales):
    mean_sq = lax.optimization_barrier(jnp.mean(inputs * inputs, axis=-1, keepdims=True))
    return inputs * lax.rsqrt(mean_sq + EPSILON) * scales

def rotate(inputs, positions):
    half_dim = inputs.shape[-1] // 2
    frequency = 10000.0 ** (-jnp.arange(half_dim, dtype=jnp.float32) / half_dim)
    angles = positions.astype(jnp.float32)[:, None] * frequency[None, :]
    cosines = jnp.cos(angles)[:, None, :]
    sines = jnp.sin(angles)[:, None, :]
    front = inputs[..., :half_dim]
    second = inputs[..., half_dim:]
    return jnp.concatenate([front * cosines - second * sines, second * cosines + front * sines], axis=-1)

def reference(hidden_in, stretch_start, pre_gain, q_weight, k_weight, v_weight, o_weight, q_gain, k_gain, prior_keys, prior_values, post_gain):
    residual_in = hidden_in.astype(jnp.float32)
    normed = rms_scale(residual_in, pre_gain).astype(jnp.bfloat16)
    positions = WINDOW + jnp.arange(TOKENS, dtype=jnp.int32)
    query_raw = jnp.dot(normed, q_weight, preferred_element_type=jnp.float32).reshape(TOKENS, HEADS, HD)
    query = (rotate(rms_scale(query_raw, q_gain), positions) * QUERY_FACTOR).astype(jnp.bfloat16)
    key_raw = jnp.dot(normed, k_weight, preferred_element_type=jnp.float32).reshape(TOKENS, KVH, HD)
    key_rows = rotate(rms_scale(key_raw, k_gain), positions).astype(jnp.bfloat16).reshape(TOKENS, KVH * HD)
    value_rows = jnp.dot(normed, v_weight, preferred_element_type=jnp.float32).astype(jnp.bfloat16)
    all_keys = jnp.concatenate([prior_keys, key_rows], axis=0)
    all_values = jnp.concatenate([prior_values, value_rows], axis=0)
    first_valid = WINDOW - stretch_start[0]
    group = HEADS // KVH
    span = WINDOW + TOK_DEV

    def one_block(block_index):
        offset = (block_index * TOK_DEV).astype(jnp.int32)
        query_block = lax.dynamic_slice_in_dim(query, offset, TOK_DEV, 0).astype(jnp.float32)
        key_block = lax.dynamic_slice_in_dim(all_keys, offset, span, 0).reshape(span, KVH, HD)
        value_block = lax.dynamic_slice_in_dim(all_values, offset, span, 0).reshape(span, KVH, HD)
        key_block = jnp.repeat(key_block, group, axis=1).astype(jnp.float32)
        value_block = jnp.repeat(value_block, group, axis=1).astype(jnp.float32)
        scores = jnp.einsum('qhd,khd->hqk', query_block, key_block)
        query_pos = WINDOW + offset + jnp.arange(TOK_DEV, dtype=jnp.int32)
        key_pos = offset + jnp.arange(span, dtype=jnp.int32)
        allowed = (key_pos[None, :] <= query_pos[:, None]) & (key_pos[None, :] > query_pos[:, None] - WINDOW) & (key_pos[None, :] >= first_valid)
        scores = jnp.where(allowed[None, :, :], scores, jnp.float32(-1e+30))
        largest = lax.optimization_barrier(jnp.max(scores, axis=-1, keepdims=True))
        expon = jnp.exp(scores - largest)
        attn_probs = (expon / lax.optimization_barrier(jnp.sum(expon, axis=-1, keepdims=True))).astype(jnp.bfloat16)
        attended = jnp.einsum('hqk,khd->qhd', attn_probs.astype(jnp.float32), value_block)
        return attended.astype(jnp.bfloat16).reshape(TOK_DEV, HEADS * HD)
    blocks = lax.map(one_block, jnp.arange(TOKENS // TOK_DEV, dtype=jnp.int32))
    attended = blocks.reshape(TOKENS, HEADS * HD)
    projected = jnp.dot(attended, o_weight, preferred_element_type=jnp.float32)
    return (residual_in + rms_scale(projected, post_gain)).astype(jnp.bfloat16)
```

```python
import functools

import jax
import jax.numpy as jnp
from jax import lax
from jax.experimental import pallas as pl
from jax.experimental.pallas import tpu as pltpu
from jax.sharding import PartitionSpec as P

HD = 128
WINDOW = 1024
EPSILON = 1e-06
QUERY_FACTOR = 168.0 ** (-0.5)


def rms_scale(inputs, scales):
    mean_sq = jnp.mean(inputs * inputs, axis=-1, keepdims=True)
    return inputs * lax.rsqrt(mean_sq + EPSILON) * scales


def norm_rope(value, gain, cosines, sines):
    normed = rms_scale(value, gain)
    return normed * cosines + pltpu.roll(normed, HD // 2, 1) * sines


def key_kernel(own_ref, other_ref, gain_ref, cos_ref, sin_ref, out_ref):
    value = own_ref[...] + other_ref[...].astype(jnp.float32)
    out_ref[...] = norm_rope(value, gain_ref[...], cos_ref[...], sin_ref[...]).astype(jnp.bfloat16)


def finish_keys(own, other, gain, cosines, sines):
    rows, cols = own.shape
    head = pl.BlockSpec((rows, HD), lambda h: (0, h))
    table = pl.BlockSpec((rows, HD), lambda h: (0, 0))
    return pl.pallas_call(
        key_kernel,
        grid=(cols // HD,),
        in_specs=[head, head, pl.BlockSpec((1, HD), lambda h: (0, 0)), table, table],
        out_specs=head,
        out_shape=jax.ShapeDtypeStruct((rows, cols), jnp.bfloat16),
        cost_estimate=pl.CostEstimate(
            flops=rows * cols * 3000, bytes_accessed=rows * cols * 8, transcendentals=0
        ),
        name="finish_keys",
    )(own, other, gain, cosines, sines)


def attend_kernel(
    group, tile, parts, first_ref, own_ref, other_ref, gain_ref, cos_ref, sin_ref, *refs
):
    key_refs, value_refs = refs[:parts], refs[parts : 2 * parts]
    out_ref, keys, values = refs[2 * parts :]
    rows = key_refs[0].shape[0]
    step = pl.program_id(1)

    @pl.when(step == 0)
    def _():
        for index in range(parts):
            keys[index * rows : (index + 1) * rows, :] = key_refs[index][...]
            values[index * rows : (index + 1) * rows, :] = value_refs[index][...]

    width = WINDOW + tile
    start = pl.multiple_of(step * tile, tile)
    heads = []
    for index in range(group):
        lanes = slice(index * HD, (index + 1) * HD)
        value = own_ref[:, lanes] + other_ref[:, lanes].astype(jnp.float32)
        turned = norm_rope(value, gain_ref[...], cos_ref[...], sin_ref[...])
        heads.append((turned * QUERY_FACTOR).astype(jnp.bfloat16))
    query = jnp.concatenate(heads, axis=0)
    scores = lax.dot_general(
        query,
        keys[pl.ds(start, width), :],
        (((1,), (1,)), ((), ())),
        preferred_element_type=jnp.float32,
    )
    row = lax.rem(lax.broadcasted_iota(jnp.int32, scores.shape, 0), tile)
    col = lax.broadcasted_iota(jnp.int32, scores.shape, 1)
    ahead = col - row
    allowed = (ahead <= WINDOW) & (ahead > 0) & (col >= first_ref[0] - start)
    scores = jnp.where(allowed, scores, jnp.float32(-1e30))
    largest = jnp.max(scores, axis=-1, keepdims=True)
    expon = jnp.exp(scores - largest)
    total = jnp.sum(expon, axis=-1, keepdims=True)
    mixed = jnp.dot(
        expon.astype(jnp.bfloat16),
        values[pl.ds(start, width), :],
        preferred_element_type=jnp.float32,
    )
    mixed = (mixed / total).astype(jnp.bfloat16)
    for index in range(group):
        out_ref[:, index * HD : (index + 1) * HD] = mixed[index * tile : (index + 1) * tile]


def attend(first, own, other, gain, cosines, sines, keys, values, kv_start, group):
    rows, cols = own.shape
    heads = cols // (HD * group)
    tile = min(256, rows)
    parts = len(keys)
    query = pl.BlockSpec((tile, group * HD), lambda h, t: (t, h))
    table = pl.BlockSpec((tile, HD), lambda h, t: (t, 0))
    kv = pl.BlockSpec((rows, HD), lambda h, t: (0, h + kv_start))
    flops = 4 * rows * group * heads * (WINDOW + tile) * HD
    return pl.pallas_call(
        functools.partial(attend_kernel, group, tile, parts),
        grid=(heads, rows // tile),
        in_specs=[
            pl.BlockSpec(memory_space=pltpu.SMEM),
            query,
            query,
            pl.BlockSpec((1, HD), lambda h, t: (0, 0)),
            table,
            table,
            *[kv] * (2 * parts),
        ],
        out_specs=query,
        out_shape=jax.ShapeDtypeStruct((rows, cols), jnp.bfloat16),
        scratch_shapes=[
            pltpu.VMEM((parts * rows, HD), jnp.bfloat16),
            pltpu.VMEM((parts * rows, HD), jnp.bfloat16),
        ],
        cost_estimate=pl.CostEstimate(
            flops=flops * 3, bytes_accessed=rows * cols * 8, transcendentals=0
        ),
        name="attend",
    )(first, own, other, gain, cosines, sines, *keys, *values)


def solution(mesh):
    n_ctx = mesh.shape["ctx"]
    n_tp = mesh.shape["tp"]
    n_core = 2
    n_y = n_tp // n_core
    n_x = n_y
    n_zj = 2
    n_zi = n_ctx // (n_x * n_zj)
    n_gather = n_zi * n_x

    def place(index):
        return index // (n_x * n_zj), (index // n_x) % n_zj, index % n_x

    def index_of(zi, zj, x):
        return (zi * n_zj + zj) * n_x + x

    def along_ctx(move):
        return [(src, index_of(*move(*place(src)))) for src in range(n_ctx)]

    to_zi = along_ctx(lambda zi, zj, x: ((zi + 1) % n_zi, zj, x))
    to_x = along_ctx(lambda zi, zj, x: (zi, zj, (x + 1) % n_x))
    to_zj = along_ctx(lambda zi, zj, x: (zi, 1 - zj, x))
    to_core = [(src, src ^ 1) for src in range(n_tp)]

    def to_y(steps):
        return [
            (src, ((src // n_core + steps) % n_y) * n_core + src % n_core) for src in range(n_tp)
        ]

    def ring(value, axis, pairs, count):
        parts = [value]
        for _ in range(count - 1):
            parts.append(lax.ppermute(parts[-1], axis, pairs))
        return parts

    def after(value, other):
        return lax.optimization_barrier((value, other))[0]

    def local(
        hidden_in,
        stretch_start,
        pre_gain,
        q_weight,
        k_weight,
        v_weight,
        o_weight,
        q_gain,
        k_gain,
        prior_keys,
        prior_values,
        post_gain,
    ):
        me = lax.axis_index("ctx")
        my_tp = lax.axis_index("tp")
        my_y, my_core = my_tp // n_core, lax.rem(my_tp, n_core)
        my_zi, my_zj, my_x = me // (n_x * n_zj), lax.rem(me // n_x, n_zj), lax.rem(me, n_x)
        tokens, width = hidden_in.shape
        block = q_weight.shape[0]
        kv_cols = k_weight.shape[1]
        q_cols = q_weight.shape[1]
        half = q_cols // 2

        def from_zi(steps):
            return lax.rem(my_zi + n_zi - steps, n_zi)

        def from_x(steps):
            return lax.rem(my_x + n_x - steps, n_x)

        residual_in = hidden_in.astype(jnp.float32)
        normed = rms_scale(residual_in, pre_gain).astype(jnp.bfloat16)

        def columns(zj):
            starts = [
                index_of(from_zi(a), zj, from_x(k)) * block
                for a in range(n_zi)
                for k in range(n_x)
            ]
            return jnp.concatenate(
                [lax.dynamic_slice_in_dim(normed, start, block, 1) for start in starts], axis=1
            )

        own_cols = columns(my_zj)
        other_cols = lax.ppermute(columns(1 - my_zj), "ctx", to_zj)

        def gather_rows(value):
            over_y = ring(value, "tp", to_y(1), n_y)
            ordered = [
                over_y[0]
                if n_y == 1
                else lax.select_n(lax.rem(my_y + n_y - y, n_y) , *over_y)
                if n_y > 2
                else jnp.where(my_y == y, over_y[0], over_y[1])
                for y in range(n_y)
            ]
            mine = jnp.stack(ordered, axis=0)
            theirs = lax.ppermute(mine, "tp", to_core)
            pair = [jnp.where(my_core == core, mine, theirs) for core in range(n_core)]
            return jnp.stack(pair, axis=1).reshape(n_tp * tokens, value.shape[1])

        rows_own = gather_rows(own_cols)
        rows_other = gather_rows(other_cols)
        row_count = rows_own.shape[0]

        o_turned = o_weight.T
        chunks = [
            v_weight,
            k_weight,
            q_weight[:, :half],
            q_weight[:, half:],
            o_turned[:, :half],
            o_turned[:, half:],
        ]
        gathered = []
        sent = []
        for index, chunk in enumerate(chunks):
            if index >= 2:
                chunk = after(chunk, sent[index - 2])
            over_zi = ring(chunk, "ctx", to_zi, n_zi)
            sent.append(over_zi[-1])
            parts = []
            for part in over_zi:
                parts.extend(ring(part, "ctx", to_x, n_x))
            gathered.append(jnp.concatenate(parts, axis=0))
        v_all, k_all, q_first, q_second, o_first, o_second = gathered

        def project(weights):
            theirs = jnp.dot(rows_other, weights, preferred_element_type=jnp.float32)
            theirs = lax.ppermute(theirs.astype(jnp.bfloat16), "ctx", to_zj)
            return jnp.dot(rows_own, weights, preferred_element_type=jnp.float32), theirs

        positions = WINDOW + me * row_count + jnp.arange(row_count, dtype=jnp.int32)
        half_dim = HD // 2
        frequency = 10000.0 ** (-jnp.arange(half_dim, dtype=jnp.float32) / half_dim)
        angles = positions.astype(jnp.float32)[:, None] * frequency[None, :]
        cosines, sines = jnp.cos(angles), jnp.sin(angles)
        cosines = jnp.concatenate([cosines, cosines], axis=1)
        sines = jnp.concatenate([-sines, sines], axis=1)

        v_own, v_other = project(v_all)
        value_rows = (v_own + v_other.astype(jnp.float32)).astype(jnp.bfloat16)
        k_own, k_other = project(k_all)
        key_rows = finish_keys(k_own, k_other, k_gain[None, :], cosines, sines)

        reach = WINDOW // row_count

        def behind(value):
            if n_x == 2 and reach == 2:
                shift = [(src, src + n_x) for src in range(n_ctx - n_x)]
                second = lax.ppermute(value, "ctx", shift)
                return [lax.ppermute(jnp.where(my_x == 0, value, second), "ctx", to_x), second]
            return [
                lax.ppermute(value, "ctx", [(src, src + hop) for src in range(n_ctx - hop)])
                for hop in range(1, reach + 1)
            ]

        def spans(rows, prior):
            earlier = behind(rows)
            parts = []
            for hop in range(reach, 0, -1):
                offset = jnp.maximum(WINDOW + (me - hop) * row_count, 0)
                cached = lax.dynamic_slice_in_dim(prior, offset, row_count, 0)
                parts.append(jnp.where(me < hop, cached, earlier[hop - 1]))
            return [*parts, rows]

        values = spans(value_rows, prior_values)
        keys = spans(key_rows, prior_keys)
        anchor = WINDOW + (me - reach) * row_count
        first = (WINDOW - stretch_start - anchor).astype(jnp.int32)
        group = q_cols // kv_cols

        attended = []
        for index, weights in enumerate((q_first, q_second)):
            q_own, q_other = project(weights)
            attended.append(
                attend(
                    first,
                    q_own,
                    q_other,
                    q_gain[None, :],
                    cosines,
                    sines,
                    keys,
                    values,
                    index * (half // (HD * group)),
                    group,
                )
            )
        attended_other = [lax.ppermute(part, "ctx", to_zj) for part in attended]

        def mix(parts):
            return sum(
                lax.dot_general(
                    part, turned, (((1,), (1,)), ((), ())), preferred_element_type=jnp.float32
                )
                for part, turned in zip(parts, (o_first, o_second))
            ).astype(jnp.bfloat16)

        def add_up(partial):
            split = partial.reshape(n_y, n_core, tokens, partial.shape[1])
            mine = lax.dynamic_index_in_dim(split, my_core, 1, keepdims=False)
            theirs = lax.dynamic_index_in_dim(split, 1 - my_core, 1, keepdims=False)
            theirs = lax.ppermute(theirs, "tp", to_core)
            summed = mine.astype(jnp.float32) + theirs.astype(jnp.float32)
            total = lax.dynamic_index_in_dim(summed, my_y, 0, keepdims=False)
            for steps in range(1, n_y):
                piece = lax.dynamic_index_in_dim(
                    summed, lax.rem(my_y + steps, n_y), 0, keepdims=False
                )
                total = total + lax.ppermute(
                    piece.astype(jnp.bfloat16), "tp", to_y(steps)
                ).astype(jnp.float32)
            return total

        own_total = add_up(mix(attended))
        other_total = add_up(mix(attended_other)).astype(jnp.bfloat16)
        back = lax.ppermute(other_total, "ctx", to_zj).astype(jnp.float32)
        relative = jnp.concatenate([own_total, back], axis=1)
        ordered = []
        for index in range(n_ctx):
            zi, zj, x = place(index)
            slot = (
                jnp.where(my_zj == zj, 0, n_gather)
                + lax.rem(my_zi + n_zi - zi, n_zi) * n_x
                + lax.rem(my_x + n_x - x, n_x)
            )
            ordered.append(lax.dynamic_slice_in_dim(relative, slot * block, block, 1))
        summed = jnp.concatenate(ordered, axis=1)
        return (residual_in + rms_scale(summed, post_gain)).astype(jnp.bfloat16)

    return jax.shard_map(
        local,
        mesh=mesh,
        in_specs=(
            P(("ctx", "tp"), None),
            P(),
            P(),
            P("ctx", "tp"),
            P("ctx", "tp"),
            P("ctx", "tp"),
            P("tp", "ctx"),
            P(),
            P(),
            P(None, "tp"),
            P(None, "tp"),
            P(),
        ),
        out_specs=P(("ctx", "tp"), None),
        check_vma=False,
    )
```
